32 devices in a mesh: batch: 1 (over z), cols: 4 (over y), rows: 8 (over x, core).
Axes of the slice: x: 4, y: 4, z: 1, core: 2. Of those that a mesh axis runs over, the one named last changes fastest.
The devices are a block of a 4x4x8 slice.
Arguments:
- frames: bfloat16 [4, 2, 64, 96, 256], P(None, 'batch', 'rows', 'cols')
- w_x: bfloat16 [3, 3, 256, 1536], replicated
- w_h: bfloat16 [3, 3, 384, 1536], replicated
- gate_bias: float32 [1536], replicated
- h_init: bfloat16 [2, 64, 96, 384], P('batch', 'rows', 'cols')
- c_init: float32 [2, 64, 96, 384], P('batch', 'rows', 'cols')
Outputs:
- output 1: bfloat16 [4, 2, 64, 96, 384], P(None, 'batch', 'rows', 'cols')
- output 2: float32 [2, 64, 96, 384], P('batch', 'rows', 'cols')
All inputs are finite; a program needn't handle non-finite values.
Results may differ from the reference program's by a relative error of at most 0.001.
Values are sent between devices in bfloat16 or wider.
A program may use at most 768 MiB of HBM per device.

```python
import jax
import jax.numpy as jnp
from jax import lax

STEPS = 4
SAMPLES = 2
GRID_HEIGHT = 64
GRID_WIDTH = 96
IN_CHANNELS = 256
HIDDEN = 384
BAND_ROWS = 8


def setup_inputs(seed: int = 0, part: int = 0) -> dict:
    root_key = jax.random.key(seed)
    shared_key, local_root = jax.random.split(root_key)
    local_key = jax.random.fold_in(local_root, part)
    key_wx, key_wh, key_bias = jax.random.split(shared_key, 3)
    key_frames, key_hidden, key_cell = jax.random.split(local_key, 3)
    gate_width = 4 * HIDDEN
    frames = jax.random.normal(key_frames, (STEPS, SAMPLES, GRID_HEIGHT, GRID_WIDTH, IN_CHANNELS), jnp.float32)
    w_x = jax.random.normal(key_wx, (3, 3, IN_CHANNELS, gate_width), jnp.float32) * (0.8 * (9 * IN_CHANNELS) ** -0.5)
    w_h = jax.random.normal(key_wh, (3, 3, HIDDEN, gate_width), jnp.float32) * (1.5 * (9 * HIDDEN) ** -0.5)
    forget_shift = jnp.concatenate([jnp.zeros((HIDDEN,), jnp.float32), jnp.ones((HIDDEN,), jnp.float32), jnp.zeros((2 * HIDDEN,), jnp.float32)])
    gate_bias = 0.5 * jax.random.normal(key_bias, (gate_width,), jnp.float32) + forget_shift
    h_init = 0.5 * jax.random.normal(key_hidden, (SAMPLES, GRID_HEIGHT, GRID_WIDTH, HIDDEN), jnp.float32)
    c_init = jax.random.normal(key_cell, (SAMPLES, GRID_HEIGHT, GRID_WIDTH, HIDDEN), jnp.float32)
    return {"frames": frames.astype(jnp.bfloat16), "w_x": w_x.astype(jnp.bfloat16), "w_h": w_h.astype(jnp.bfloat16), "gate_bias": gate_bias, "h_init": h_init.astype(jnp.bfloat16), "c_init": c_init}


def conv_taps(padded, weights, out_rows, out_cols):
    tap_list = [padded[:, row_off:row_off + out_rows, col_off:col_off + out_cols, :] for row_off in range(3) for col_off in range(3)]
    patches = jnp.concatenate(tap_list, axis=-1)
    flat_patches = patches.reshape(-1, patches.shape[-1])
    flat_weights = weights.reshape(-1, weights.shape[-1])
    product = jnp.dot(flat_patches, flat_weights, preferred_element_type=jnp.float32)
    return product.reshape(padded.shape[0], out_rows, out_cols, -1)


def lstm_cell(gate_sum, cell_prev):
    hidden_width = cell_prev.shape[-1]
    in_gate = jax.nn.sigmoid(gate_sum[..., :hidden_width])
    forget_gate = jax.nn.sigmoid(gate_sum[..., hidden_width:2 * hidden_width])
    out_gate = jax.nn.sigmoid(gate_sum[..., 2 * hidden_width:3 * hidden_width])
    cand_gate = jnp.tanh(gate_sum[..., 3 * hidden_width:])
    cell_next = forget_gate * cell_prev + in_gate * cand_gate
    hidden_next = (out_gate * jnp.tanh(cell_next)).astype(jnp.bfloat16)
    return hidden_next, cell_next


def reference(frames, w_x, w_h, gate_bias, h_init, c_init):
    num_bands = GRID_HEIGHT // BAND_ROWS
    pad_cfg = ((0, 0), (1, 1), (1, 1), (0, 0))

    def step_fn(state_pair, frame_t):
        hidden, cell_state = state_pair
        frame_pad = jnp.pad(frame_t, pad_cfg)
        hidden_pad = jnp.pad(hidden, pad_cfg)

        def band_update(band_index):
            row_start = band_index * BAND_ROWS
            frame_band = lax.dynamic_slice_in_dim(frame_pad, row_start, BAND_ROWS + 2, axis=1)
            hidden_band = lax.dynamic_slice_in_dim(hidden_pad, row_start, BAND_ROWS + 2, axis=1)
            cell_band = lax.dynamic_slice_in_dim(cell_state, row_start, BAND_ROWS, axis=1)
            gate_sum = conv_taps(frame_band, w_x, BAND_ROWS, GRID_WIDTH) + conv_taps(hidden_band, w_h, BAND_ROWS, GRID_WIDTH) + gate_bias
            return lstm_cell(gate_sum, cell_band)

        band_hidden, band_cell = lax.map(band_update, jnp.arange(num_bands))
        hidden_next = jnp.moveaxis(band_hidden, 0, 1).reshape(SAMPLES, GRID_HEIGHT, GRID_WIDTH, HIDDEN)
        cell_next = jnp.moveaxis(band_cell, 0, 1).reshape(SAMPLES, GRID_HEIGHT, GRID_WIDTH, HIDDEN)
        return (hidden_next, cell_next), hidden_next

    final_pair, all_hidden = lax.scan(step_fn, (h_init, c_init), frames)
    return all_hidden, final_pair[1]
```

```python
import jax
import jax.numpy as jnp
from jax import lax
from jax.experimental import pallas as pl
from jax.experimental.pallas import tpu as pltpu
from jax.sharding import PartitionSpec as P

MESH = pl.DeviceIdType.MESH
LANES = 128
SLOTS = ((-1, 0), (1, 0), (0, -1), (0, 1), (-1, -1), (-1, 1), (1, -1), (1, 1))


def sigmoid(x):
    return 0.5 * jnp.tanh(0.5 * x) + 0.5


def make_kernel(dims, row_count, col_count):
    T, SEQ, H, W, CX, CH = dims
    PR = SEQ * W
    M = H * PR
    NJ = CH // LANES

    def kernel(frames, wx_hbm, wh_hbm, bias_hbm, h_init, c_init, h_out, c_out,
               wx, wh, bias, rawx, rawh, cst, sx, sh, g, hf, ho, ecx, ech, acx, ach,
               wsem, rsem, osem, xsend, xrecv, hsend, hrecv):
        b = lax.axis_index("batch")
        row = lax.axis_index("rows")
        col = lax.axis_index("cols")

        def exists(dr, dc):
            r, c = row + dr, col + dc
            return (r >= 0) & (r < row_count) & (c >= 0) & (c < col_count)

        barrier = pltpu.get_barrier_semaphore()
        for dr, dc in SLOTS:
            @pl.when(exists(dr, dc))
            def _():
                pl.semaphore_signal(barrier, inc=1, device_id=(b, col + dc, row + dr), device_id_type=MESH)

        xloads = [[pltpu.make_async_copy(frames.at[t, s], rawx.at[t, :, s], rsem.at[t, s]) for s in range(SEQ)]
                  for t in range(T)]
        hloads = [pltpu.make_async_copy(h_init.at[s], rawh.at[:, s], rsem.at[T, s]) for s in range(SEQ)]
        cloads = [pltpu.make_async_copy(c_init.at[s], cst.at[:, s], rsem.at[T + 1, s]) for s in range(SEQ)]
        bload = pltpu.make_async_copy(bias_hbm, bias, wsem.at[2])
        wxload = pltpu.make_async_copy(wx_hbm, wx, wsem.at[0])
        whload = pltpu.make_async_copy(wh_hbm, wh, wsem.at[1])
        for t in range(T):
            for cp in xloads[t]:
                cp.start()
        for cp in hloads:
            cp.start()
        bload.start()
        wxload.start()
        for cp in cloads:
            cp.start()
        whload.start()

        def zero(cond, refs):
            @pl.when(cond)
            def _():
                for ref in refs:
                    ref[...] = jnp.zeros(ref.shape, ref.dtype)
        zero(row == 0, [sx.at[:, 1, 0:PR], sh.at[:, 1, 0:PR], acx.at[:, :, 0], ach.at[:, :, 0]])
        zero(row == row_count - 1, [sx.at[:, 1, M + PR:M + 2 * PR], sh.at[:, 1, M + PR:M + 2 * PR],
                                    acx.at[:, :, H + 1], ach.at[:, :, H + 1]])
        zero(col == 0, [acx.at[:, 0], ach.at[:, 0]])
        zero(col == col_count - 1, [acx.at[:, 1], ach.at[:, 1]])

        def copies(s_t, ec_t, ac_t, send, recv):
            s0 = s_t.at[1]
            parts = ((s0.at[pl.ds(M, PR)], s0.at[pl.ds(0, PR)]),
                     (s0.at[pl.ds(PR, PR)], s0.at[pl.ds(M + PR, PR)]),
                     (ec_t.at[1], ac_t.at[0, pl.ds(1, H)]),
                     (ec_t.at[0], ac_t.at[1, pl.ds(1, H)]),
                     (ec_t.at[1, H - 1], ac_t.at[0, 0]),
                     (ec_t.at[0, H - 1], ac_t.at[1, 0]),
                     (ec_t.at[1, 0], ac_t.at[0, H + 1]),
                     (ec_t.at[0, 0], ac_t.at[1, H + 1]))
            out = []
            for i, (dr, dc) in enumerate(SLOTS):
                cp = pltpu.make_async_remote_copy(
                    src_ref=parts[i][0], dst_ref=parts[i][1], send_sem=send.at[i], recv_sem=recv.at[i],
                    device_id=(b, col - dc, row - dr), device_id_type=MESH)
                out.append((exists(-dr, -dc), exists(dr, dc), cp))
            return out

        def start_all(cps):
            for can_send, _, cp in cps:
                @pl.when(can_send)
                def _():
                    cp.start()

        def wait_recv_all(cps):
            for _, can_recv, cp in cps:
                @pl.when(can_recv)
                def _():
                    cp.wait_recv()

        def wait_send_all(cps):
            for can_send, _, cp in cps:
                @pl.when(can_send)
                def _():
                    cp.wait_send()

        def xcopies(t):
            return copies(sx.at[t], ecx.at[t], acx.at[t], xsend.at[t], xrecv.at[t])

        def hcopies(t):
            return copies(sh.at[t], ech.at[t], ach.at[t], hsend.at[t], hrecv.at[t])

        def shifted(v):
            n = v.shape[0]
            c_idx = lax.broadcasted_iota(jnp.int32, v.shape, 0) % W
            left = jnp.where(c_idx == 0, 0.0, pltpu.roll(v, 1, 0))
            right = jnp.where(c_idx == W - 1, 0.0, pltpu.roll(v, n - 1, 0))
            return left, right

        def put_tile(s_ref, ec_ref, v, lane):
            left, right = shifted(v)
            s_ref[0, pl.ds(PR, M), pl.ds(lane, LANES)] = left.astype(jnp.bfloat16)
            s_ref[1, pl.ds(PR, M), pl.ds(lane, LANES)] = v.astype(jnp.bfloat16)
            s_ref[2, pl.ds(PR, M), pl.ds(lane, LANES)] = right.astype(jnp.bfloat16)
            j = lane // LANES
            hf[j] = v
            first = hf[j, pl.ds(0, H * SEQ, stride=W), :]
            last = hf[j, pl.ds(W - 1, H * SEQ, stride=W), :]
            ec_ref[0, :, :, pl.ds(lane, LANES)] = first.astype(jnp.bfloat16).reshape(H, SEQ, LANES)
            ec_ref[1, :, :, pl.ds(lane, LANES)] = last.astype(jnp.bfloat16).reshape(H, SEQ, LANES)

        def patch(s_ref, ac_ref, channels):
            i16 = lax.broadcasted_iota(jnp.int32, (16, channels), 0)
            for r in range(H):
                for side in range(2):
                    for s in range(SEQ):
                        pos = s * W if side == 0 else s * W + W - 1
                        base = PR * (r + 1) + pos // 16 * 16
                        dxi = 2 * side
                        old = s_ref[dxi, pl.ds(base, 16), :].astype(jnp.float32)
                        halo = ac_ref[side, r + 1, s:s + 1, :].astype(jnp.float32)
                        s_ref[dxi, pl.ds(base, 16), :] = jnp.where(i16 == pos % 16, halo, old).astype(jnp.bfloat16)
            pos_idx = lax.broadcasted_iota(jnp.int32, (PR, channels), 0)
            for r in (0, H + 1):
                v = s_ref[1, pl.ds(PR * r, PR), :].astype(jnp.float32)
                for side in range(2):
                    out = pltpu.roll(v, 1 if side == 0 else PR - 1, 0)
                    for s in range(SEQ):
                        halo = ac_ref[side, r, s:s + 1, :].astype(jnp.float32)
                        out = jnp.where(pos_idx == (s * W if side == 0 else s * W + W - 1), halo, out)
                    s_ref[2 * side, pl.ds(PR * r, PR), :] = out.astype(jnp.bfloat16)

        def conv(s_ref, w_ref, j):
            lhs = jnp.concatenate([s_ref[dx, pl.ds(dy * PR, M), :] for dy in range(3) for dx in range(3)], axis=1)
            rhs = jnp.concatenate([w_ref[:, pl.ds(q * CH + j * LANES, LANES)] for q in range(4)], axis=1)
            return jnp.dot(lhs, rhs, preferred_element_type=jnp.float32)

        def x_phase(t):
            for j in range(NJ):
                bj = jnp.concatenate([bias[:, pl.ds(q * CH + j * LANES, LANES)] for q in range(4)], axis=1)
                g[j] = conv(sx.at[t], wx, j) + bj

        def out_copies(t):
            return [pltpu.make_async_copy(ho.at[t, s], h_out.at[t, s], osem.at[t, s]) for s in range(SEQ)]

        def h_phase(t, last):
            for j in range(NJ):
                lane = j * LANES
                gates = conv(sh.at[t], wh, j) + g[j]
                gi = sigmoid(gates[:, 0:LANES])
                gf = sigmoid(gates[:, LANES:2 * LANES])
                go = sigmoid(gates[:, 2 * LANES:3 * LANES])
                gg = jnp.tanh(gates[:, 3 * LANES:])
                c_old = cst[:, :, :, pl.ds(lane, LANES)].reshape(M, LANES)
                c_new = gf * c_old + gi * gg
                cst[:, :, :, pl.ds(lane, LANES)] = c_new.reshape(H, SEQ, W, LANES)
                h_new = go * jnp.tanh(c_new)
                h4 = h_new.reshape(H, SEQ, W, LANES)
                for s in range(SEQ):
                    ho[t, s, :, :, pl.ds(lane, LANES)] = h4[:, s].astype(jnp.bfloat16)
                if not last:
                    put_tile(sh.at[t + 1], ech.at[t + 1], h_new, lane)

        def fill(raw, s_ref, ec_ref, channels):
            for k in range(channels // LANES):
                lane = k * LANES
                v = raw[:, :, :, pl.ds(lane, LANES)].astype(jnp.float32).reshape(M, LANES)
                put_tile(s_ref, ec_ref, v, lane)

        for cp in xloads[0]:
            cp.wait()
        fill(rawx.at[0], sx.at[0], ecx.at[0], CX)
        for cp in hloads:
            cp.wait()
        fill(rawh, sh.at[0], ech.at[0], CH)
        n_near = sum(exists(dr, dc).astype(jnp.int32) for dr, dc in SLOTS)
        pl.semaphore_wait(barrier, n_near)
        start_all(xcopies(0))
        start_all(hcopies(0))
        for t in range(1, T):
            for cp in xloads[t]:
                cp.wait()

        @pl.loop(1, T)
        def _(t):
            fill(rawx.at[t], sx.at[t], ecx.at[t], CX)
            start_all(xcopies(t))

        bload.wait()
        for cp in cloads:
            cp.wait()
        wait_recv_all(xcopies(0))
        patch(sx.at[0], acx.at[0], CX)
        wxload.wait()
        x_phase(0)
        whload.wait()

        @pl.loop(0, T - 1)
        def _(t):
            wait_recv_all(hcopies(t))
            patch(sh.at[t], ach.at[t], CH)
            h_phase(t, False)
            for cp in out_copies(t):
                cp.start()
            start_all(hcopies(t + 1))
            wait_recv_all(xcopies(t + 1))
            patch(sx.at[t + 1], acx.at[t + 1], CX)
            x_phase(t + 1)

        wait_recv_all(hcopies(T - 1))
        patch(sh.at[T - 1], ach.at[T - 1], CH)
        h_phase(T - 1, True)
        for cp in out_copies(T - 1):
            cp.start()
        c_copies = [pltpu.make_async_copy(cst.at[:, s], c_out.at[s], osem.at[T, s]) for s in range(SEQ)]
        for cp in c_copies:
            cp.start()
        for t in range(T):
            wait_send_all(xcopies(t))
            wait_send_all(hcopies(t))
            for cp in out_copies(t):
                cp.wait()
        for cp in c_copies:
            cp.wait()

    return kernel


def solution(mesh):
    row_count = mesh.shape["rows"]
    col_count = mesh.shape["cols"]
    frame_spec = P(None, "batch", "rows", "cols", None)
    state_spec = P("batch", "rows", "cols", None)

    def local_run(frames, w_x, w_h, gate_bias, h_init, c_init):
        T, SEQ, H, W, CX = frames.shape
        CH = h_init.shape[-1]
        NG = 4 * CH
        PR = SEQ * W
        M = H * PR
        bf, f32 = jnp.bfloat16, jnp.float32
        hbm = pl.BlockSpec(memory_space=pl.ANY)
        kernel = make_kernel((T, SEQ, H, W, CX, CH), row_count, col_count)
        return pl.pallas_call(
            kernel,
            out_shape=(jax.ShapeDtypeStruct((T, SEQ, H, W, CH), bf), jax.ShapeDtypeStruct((SEQ, H, W, CH), f32)),
            in_specs=[hbm] * 6,
            out_specs=(hbm, hbm),
            scratch_shapes=[
                pltpu.VMEM((9 * CX, NG), bf), pltpu.VMEM((9 * CH, NG), bf), pltpu.VMEM((1, NG), f32),
                pltpu.VMEM((T, H, SEQ, W, CX), bf), pltpu.VMEM((H, SEQ, W, CH), bf), pltpu.VMEM((H, SEQ, W, CH), f32),
                pltpu.VMEM((T, 3, M + 2 * PR, CX), bf), pltpu.VMEM((T, 3, M + 2 * PR, CH), bf),
                pltpu.VMEM((CH // LANES, M, 4 * LANES), f32), pltpu.VMEM((max(CH, CX) // LANES, M, LANES), f32),
                pltpu.VMEM((T, SEQ, H, W, CH), bf),
                pltpu.VMEM((T, 2, H, SEQ, CX), bf), pltpu.VMEM((T, 2, H, SEQ, CH), bf),
                pltpu.VMEM((T, 2, H + 2, SEQ, CX), bf), pltpu.VMEM((T, 2, H + 2, SEQ, CH), bf),
                pltpu.SemaphoreType.DMA((3,)), pltpu.SemaphoreType.DMA((T + 2, SEQ)),
                pltpu.SemaphoreType.DMA((T + 1, SEQ)),
                pltpu.SemaphoreType.DMA((T, 8)), pltpu.SemaphoreType.DMA((T, 8)),
                pltpu.SemaphoreType.DMA((T, 8)), pltpu.SemaphoreType.DMA((T, 8)),
            ],
            compiler_params=pltpu.CompilerParams(
                collective_id=0, has_side_effects=True, vmem_limit_bytes=60 * 1024 * 1024),
        )(frames, w_x.reshape(9 * CX, NG), w_h.reshape(9 * CH, NG), gate_bias.reshape(1, NG), h_init, c_init)

    return jax.shard_map(local_run, mesh=mesh,
                         in_specs=(frame_spec, P(), P(), P(), state_spec, state_spec),
                         out_specs=(frame_spec, state_spec), check_vma=False)
```

```python
import jax
import jax.numpy as jnp
from jax import lax
from jax.experimental import pallas as pl
from jax.experimental.pallas import tpu as pltpu
from jax.sharding import PartitionSpec as P

MESH = pl.DeviceIdType.MESH
LANES = 128
SLOTS = ((-1, 0), (1, 0), (0, -1), (0, 1), (-1, -1), (-1, 1), (1, -1), (1, 1))


def sigmoid(x):
    return 0.5 * jnp.tanh(0.5 * x) + 0.5


def make_kernel(dims, row_count, col_count):
    T, SEQ, H, W, CX, CH = dims
    PR = SEQ * W
    M = H * PR
    NJ = CH // LANES

    def kernel(frames, wx_hbm, wh_hbm, bias_hbm, h_init, c_init, ho, cst,
               wx, wh, bias, rawx, rawh, sx, sh, g, hf, ecx, ech, acx, ach,
               wsem, rsem, xsend, xrecv, hsend, hrecv):
        b = lax.axis_index("batch")
        row = lax.axis_index("rows")
        col = lax.axis_index("cols")

        def exists(dr, dc):
            r, c = row + dr, col + dc
            return (r >= 0) & (r < row_count) & (c >= 0) & (c < col_count)

        barrier = pltpu.get_barrier_semaphore()
        for dr, dc in SLOTS:
            @pl.when(exists(dr, dc))
            def _():
                pl.semaphore_signal(barrier, inc=1, device_id=(b, col + dc, row + dr), device_id_type=MESH)

        xloads = [[pltpu.make_async_copy(frames.at[t, s], rawx.at[t, :, s], rsem.at[t, s]) for s in range(SEQ)]
                  for t in range(T)]
        hloads = [pltpu.make_async_copy(h_init.at[s], rawh.at[:, s], rsem.at[T, s]) for s in range(SEQ)]
        cloads = [pltpu.make_async_copy(c_init.at[s], cst.at[:, s], rsem.at[T + 1, s]) for s in range(SEQ)]
        bload = pltpu.make_async_copy(bias_hbm, bias, wsem.at[2])
        wxload = pltpu.make_async_copy(wx_hbm, wx, wsem.at[0])
        whload = pltpu.make_async_copy(wh_hbm, wh, wsem.at[1])
        for t in range(T):
            for cp in xloads[t]:
                cp.start()
        for cp in hloads:
            cp.start()
        bload.start()
        wxload.start()
        for cp in cloads:
            cp.start()
        whload.start()

        def zero(cond, refs):
            @pl.when(cond)
            def _():
                for ref in refs:
                    ref[...] = jnp.zeros(ref.shape, ref.dtype)
        zero(row == 0, [sx.at[:, 1, 0:PR], sh.at[:, 1, 0:PR], acx.at[:, :, 0], ach.at[:, :, 0]])
        zero(row == row_count - 1, [sx.at[:, 1, M + PR:M + 2 * PR], sh.at[:, 1, M + PR:M + 2 * PR],
                                    acx.at[:, :, H + 1], ach.at[:, :, H + 1]])
        zero(col == 0, [acx.at[:, 0], ach.at[:, 0]])
        zero(col == col_count - 1, [acx.at[:, 1], ach.at[:, 1]])

        def copies(s_t, ec_t, ac_t, send, recv):
            s0 = s_t.at[1]
            parts = ((s0.at[pl.ds(M, PR)], s0.at[pl.ds(0, PR)]),
                     (s0.at[pl.ds(PR, PR)], s0.at[pl.ds(M + PR, PR)]),
                     (ec_t.at[1], ac_t.at[0, pl.ds(1, H)]),
                     (ec_t.at[0], ac_t.at[1, pl.ds(1, H)]),
                     (ec_t.at[1, H - 1], ac_t.at[0, 0]),
                     (ec_t.at[0, H - 1], ac_t.at[1, 0]),
                     (ec_t.at[1, 0], ac_t.at[0, H + 1]),
                     (ec_t.at[0, 0], ac_t.at[1, H + 1]))
            out = []
            for i, (dr, dc) in enumerate(SLOTS):
                cp = pltpu.make_async_remote_copy(
                    src_ref=parts[i][0], dst_ref=parts[i][1], send_sem=send.at[i], recv_sem=recv.at[i],
                    device_id=(b, col - dc, row - dr), device_id_type=MESH)
                out.append((exists(-dr, -dc), exists(dr, dc), cp))
            return out

        def start_all(cps):
            for can_send, _, cp in cps:
                @pl.when(can_send)
                def _():
                    cp.start()

        def wait_recv_all(cps):
            for _, can_recv, cp in cps:
                @pl.when(can_recv)
                def _():
                    cp.wait_recv()

        def wait_send_all(cps):
            for can_send, _, cp in cps:
                @pl.when(can_send)
                def _():
                    cp.wait_send()

        def xcopies(t):
            return copies(sx.at[t], ecx.at[t], acx.at[t], xsend.at[t], xrecv.at[t])

        def hcopies(t):
            return copies(sh.at[t], ech.at[t], ach.at[t], hsend.at[t], hrecv.at[t])

        def shifted(v):
            n = v.shape[0]
            c_idx = lax.broadcasted_iota(jnp.int32, v.shape, 0) % W
            left = jnp.where(c_idx == 0, 0.0, pltpu.roll(v, 1, 0))
            right = jnp.where(c_idx == W - 1, 0.0, pltpu.roll(v, n - 1, 0))
            return left, right

        def put_tile(s_ref, ec_ref, v, lane):
            left, right = shifted(v)
            s_ref[0, pl.ds(PR, M), pl.ds(lane, LANES)] = left.astype(jnp.bfloat16)
            s_ref[1, pl.ds(PR, M), pl.ds(lane, LANES)] = v.astype(jnp.bfloat16)
            s_ref[2, pl.ds(PR, M), pl.ds(lane, LANES)] = right.astype(jnp.bfloat16)
            j = lane // LANES
            hf[j] = v
            first = hf[j, pl.ds(0, H * SEQ, stride=W), :]
            last = hf[j, pl.ds(W - 1, H * SEQ, stride=W), :]
            ec_ref[0, :, :, pl.ds(lane, LANES)] = first.astype(jnp.bfloat16).reshape(H, SEQ, LANES)
            ec_ref[1, :, :, pl.ds(lane, LANES)] = last.astype(jnp.bfloat16).reshape(H, SEQ, LANES)

        def patch(s_ref, ac_ref, channels):
            i16 = lax.broadcasted_iota(jnp.int32, (16, channels), 0)
            for r in range(H):
                for side in range(2):
                    for s in range(SEQ):
                        pos = s * W if side == 0 else s * W + W - 1
                        base = PR * (r + 1) + pos // 16 * 16
                        dxi = 2 * side
                        old = s_ref[dxi, pl.ds(base, 16), :].astype(jnp.float32)
                        halo = ac_ref[side, r + 1, s:s + 1, :].astype(jnp.float32)
                        s_ref[dxi, pl.ds(base, 16), :] = jnp.where(i16 == pos % 16, halo, old).astype(jnp.bfloat16)
            pos_idx = lax.broadcasted_iota(jnp.int32, (PR, channels), 0)
            for r in (0, H + 1):
                v = s_ref[1, pl.ds(PR * r, PR), :].astype(jnp.float32)
                for side in range(2):
                    out = pltpu.roll(v, 1 if side == 0 else PR - 1, 0)
                    for s in range(SEQ):
                        halo = ac_ref[side, r, s:s + 1, :].astype(jnp.float32)
                        out = jnp.where(pos_idx == (s * W if side == 0 else s * W + W - 1), halo, out)
                    s_ref[2 * side, pl.ds(PR * r, PR), :] = out.astype(jnp.bfloat16)

        def conv(s_ref, w_ref, j):
            lhs = jnp.concatenate([s_ref[dx, pl.ds(dy * PR, M), :] for dy in range(3) for dx in range(3)], axis=1)
            rhs = jnp.concatenate([w_ref[:, pl.ds(q * CH + j * LANES, LANES)] for q in range(4)], axis=1)
            return jnp.dot(lhs, rhs, preferred_element_type=jnp.float32)

        def x_phase(t):
            for j in range(NJ):
                bj = jnp.concatenate([bias[pl.ds(q * CH + j * LANES, LANES)].reshape(1, LANES) for q in range(4)], axis=1)
                g[j] = conv(sx.at[t], wx, j) + bj

        def h_phase(t, last):
            for j in range(NJ):
                lane = j * LANES
                gates = conv(sh.at[t], wh, j) + g[j]
                gi = sigmoid(gates[:, 0:LANES])
                gf = sigmoid(gates[:, LANES:2 * LANES])
                go = sigmoid(gates[:, 2 * LANES:3 * LANES])
                gg = jnp.tanh(gates[:, 3 * LANES:])
                c_old = cst[:, :, :, pl.ds(lane, LANES)].reshape(M, LANES)
                c_new = gf * c_old + gi * gg
                cst[:, :, :, pl.ds(lane, LANES)] = c_new.reshape(H, SEQ, W, LANES)
                h_new = go * jnp.tanh(c_new)
                h4 = h_new.reshape(H, SEQ, W, LANES)
                for s in range(SEQ):
                    ho[t, s, :, :, pl.ds(lane, LANES)] = h4[:, s].astype(jnp.bfloat16)
                if not last:
                    put_tile(sh.at[t + 1], ech.at[t + 1], h_new, lane)

        def fill(raw, s_ref, ec_ref, channels):
            for k in range(channels // LANES):
                lane = k * LANES
                v = raw[:, :, :, pl.ds(lane, LANES)].astype(jnp.float32).reshape(M, LANES)
                put_tile(s_ref, ec_ref, v, lane)

        for cp in xloads[0]:
            cp.wait()
        fill(rawx.at[0], sx.at[0], ecx.at[0], CX)
        for cp in hloads:
            cp.wait()
        fill(rawh, sh.at[0], ech.at[0], CH)
        n_near = sum(exists(dr, dc).astype(jnp.int32) for dr, dc in SLOTS)
        pl.semaphore_wait(barrier, n_near)
        start_all(xcopies(0))
        start_all(hcopies(0))
        for t in range(1, T):
            for cp in xloads[t]:
                cp.wait()

        @pl.loop(1, T)
        def _(t):
            fill(rawx.at[t], sx.at[t], ecx.at[t], CX)
            start_all(xcopies(t))

        bload.wait()
        for cp in cloads:
            cp.wait()
        wait_recv_all(xcopies(0))
        patch(sx.at[0], acx.at[0], CX)
        wxload.wait()
        x_phase(0)
        whload.wait()

        @pl.loop(0, T - 1)
        def _(t):
            wait_recv_all(hcopies(t))
            patch(sh.at[t], ach.at[t], CH)
            h_phase(t, False)
            start_all(hcopies(t + 1))
            wait_recv_all(xcopies(t + 1))
            patch(sx.at[t + 1], acx.at[t + 1], CX)
            x_phase(t + 1)

        wait_recv_all(hcopies(T - 1))
        patch(sh.at[T - 1], ach.at[T - 1], CH)
        h_phase(T - 1, True)
        for t in range(T):
            wait_send_all(xcopies(t))
            wait_send_all(hcopies(t))

    return kernel


def solution(mesh):
    row_count = mesh.shape["rows"]
    col_count = mesh.shape["cols"]
    frame_spec = P(None, "batch", "rows", "cols", None)
    state_spec = P("batch", "rows", "cols", None)

    def local_run(frames, w_x, w_h, gate_bias, h_init, c_init):
        T, SEQ, H, W, CX = frames.shape
        CH = h_init.shape[-1]
        NG = 4 * CH
        PR = SEQ * W
        M = H * PR
        bf, f32 = jnp.bfloat16, jnp.float32
        hbm = pl.BlockSpec(memory_space=pl.ANY)
        vmem = pl.BlockSpec(memory_space=pltpu.VMEM)
        kernel = make_kernel((T, SEQ, H, W, CX, CH), row_count, col_count)
        h_vmem, c_vmem = pl.pallas_call(
            kernel,
            out_shape=(pltpu.VMEM((T, SEQ, H, W, CH), bf), pltpu.VMEM((H, SEQ, W, CH), f32)),
            in_specs=[hbm] * 6,
            out_specs=(vmem, vmem),
            scratch_shapes=[
                pltpu.VMEM((9 * CX, NG), bf), pltpu.VMEM((9 * CH, NG), bf), pltpu.VMEM((NG,), f32),
                pltpu.VMEM((T, H, SEQ, W, CX), bf), pltpu.VMEM((H, SEQ, W, CH), bf),
                pltpu.VMEM((T, 3, M + 2 * PR, CX), bf), pltpu.VMEM((T, 3, M + 2 * PR, CH), bf),
                pltpu.VMEM((CH // LANES, M, 4 * LANES), f32), pltpu.VMEM((max(CH, CX) // LANES, M, LANES), f32),
                pltpu.VMEM((T, 2, H, SEQ, CX), bf), pltpu.VMEM((T, 2, H, SEQ, CH), bf),
                pltpu.VMEM((T, 2, H + 2, SEQ, CX), bf), pltpu.VMEM((T, 2, H + 2, SEQ, CH), bf),
                pltpu.SemaphoreType.DMA((3,)), pltpu.SemaphoreType.DMA((T + 2, SEQ)),
                pltpu.SemaphoreType.DMA((T, 8)), pltpu.SemaphoreType.DMA((T, 8)),
                pltpu.SemaphoreType.DMA((T, 8)), pltpu.SemaphoreType.DMA((T, 8)),
            ],
            compiler_params=pltpu.CompilerParams(
                collective_id=0, has_side_effects=True, vmem_limit_bytes=56 * 1024 * 1024),
        )(frames, w_x.reshape(9 * CX, NG), w_h.reshape(9 * CH, NG), gate_bias, h_init, c_init)

        def write_out(h_ref, c_ref, h_out, c_out, sem):
            cps = [pltpu.make_async_copy(h_ref, h_out, sem.at[SEQ])]
            cps += [pltpu.make_async_copy(c_ref.at[:, s], c_out.at[s], sem.at[s]) for s in range(SEQ)]
            for cp in cps:
                cp.start()
            for cp in cps:
                cp.wait()

        return pl.pallas_call(
            write_out,
            out_shape=(jax.ShapeDtypeStruct((T, SEQ, H, W, CH), bf), jax.ShapeDtypeStruct((SEQ, H, W, CH), f32)),
            in_specs=[vmem] * 2,
            out_specs=(hbm, hbm),
            scratch_shapes=[pltpu.SemaphoreType.DMA((SEQ + 1,))],
            compiler_params=pltpu.CompilerParams(vmem_limit_bytes=1024 * 1024),
        )(h_vmem, c_vmem)

    return jax.shard_map(local_run, mesh=mesh,
                         in_specs=(frame_spec, P(), P(), P(), state_spec, state_spec),
                         out_specs=(frame_spec, state_spec), check_vma=False)
```

```python
import jax
import jax.numpy as jnp
from jax import lax
from jax.experimental import pallas as pl
from jax.experimental.pallas import tpu as pltpu
from jax.sharding import PartitionSpec as P

MESH = pl.DeviceIdType.MESH
LANES = 128
SLOTS = ((-1, 0), (1, 0), (0, -1), (0, 1), (-1, -1), (-1, 1), (1, -1), (1, 1))


def sigmoid(x):
    return 0.5 * jnp.tanh(0.5 * x) + 0.5


def make_kernel(dims, row_count, col_count):
    T, SEQ, H, W, CX, CH = dims
    PR = SEQ * W
    M = H * PR
    NJ = CH // LANES

    def kernel(frames, wx_hbm, wh_hbm, bias_hbm, h_init, c_init, ho, cst,
               wx, wh, bias, rawx, rawh, sx, sh, g, hf, ecx, ech, acx, ach,
               wsem, rsem, xsend, xrecv, hsend, hrecv):
        b = lax.axis_index("batch")
        row = lax.axis_index("rows")
        col = lax.axis_index("cols")

        def exists(dr, dc):
            r, c = row + dr, col + dc
            return (r >= 0) & (r < row_count) & (c >= 0) & (c < col_count)

        barrier = pltpu.get_barrier_semaphore()
        for dr, dc in SLOTS:
            @pl.when(exists(dr, dc))
            def _():
                pl.semaphore_signal(barrier, inc=1, device_id=(b, col + dc, row + dr), device_id_type=MESH)

        xloads = [[pltpu.make_async_copy(frames.at[t, s], rawx.at[t, :, s], rsem.at[t, s]) for s in range(SEQ)]
                  for t in range(T)]
        hloads = [pltpu.make_async_copy(h_init.at[s], rawh.at[:, s], rsem.at[T, s]) for s in range(SEQ)]
        cloads = [pltpu.make_async_copy(c_init.at[s], cst.at[:, s], rsem.at[T + 1, s]) for s in range(SEQ)]
        bload = pltpu.make_async_copy(bias_hbm, bias, wsem.at[0])

        def wloads(w_hbm, w_vmem, channels, first_sem):
            parts = (pl.ds(4 * channels, channels), pl.ds(0, 4 * channels), pl.ds(5 * channels, 4 * channels))
            return [pltpu.make_async_copy(w_hbm.at[p], w_vmem.at[p], wsem.at[first_sem + i]) for i, p in enumerate(parts)]
        wxloads = wloads(wx_hbm, wx, CX, 1)
        whloads = wloads(wh_hbm, wh, CH, 4)
        later = [cp for t in range(1, T) for cp in xloads[t]]
        for cp in [*xloads[0], *hloads, bload, wxloads[0], whloads[0], *later, *wxloads[1:], *cloads, *whloads[1:]]:
            cp.start()

        def zero(cond, refs):
            @pl.when(cond)
            def _():
                for ref in refs:
                    ref[...] = jnp.zeros(ref.shape, ref.dtype)
        zero(row == 0, [sx.at[:, 1, 0:PR], sh.at[:, 1, 0:PR], acx.at[:, :, 0], ach.at[:, :, 0]])
        zero(row == row_count - 1, [sx.at[:, 1, M + PR:M + 2 * PR], sh.at[:, 1, M + PR:M + 2 * PR],
                                    acx.at[:, :, H + 1], ach.at[:, :, H + 1]])
        zero(col == 0, [acx.at[:, 0], ach.at[:, 0]])
        zero(col == col_count - 1, [acx.at[:, 1], ach.at[:, 1]])

        def copies(s_t, ec_t, ac_t, send, recv):
            s0 = s_t.at[1]
            parts = ((s0.at[pl.ds(M, PR)], s0.at[pl.ds(0, PR)]),
                     (s0.at[pl.ds(PR, PR)], s0.at[pl.ds(M + PR, PR)]),
                     (ec_t.at[1], ac_t.at[0, pl.ds(1, H)]),
                     (ec_t.at[0], ac_t.at[1, pl.ds(1, H)]),
                     (ec_t.at[1, H - 1], ac_t.at[0, 0]),
                     (ec_t.at[0, H - 1], ac_t.at[1, 0]),
                     (ec_t.at[1, 0], ac_t.at[0, H + 1]),
                     (ec_t.at[0, 0], ac_t.at[1, H + 1]))
            out = []
            for i, (dr, dc) in enumerate(SLOTS):
                cp = pltpu.make_async_remote_copy(
                    src_ref=parts[i][0], dst_ref=parts[i][1], send_sem=send.at[i], recv_sem=recv.at[i],
                    device_id=(b, col - dc, row - dr), device_id_type=MESH)
                out.append((exists(-dr, -dc), exists(dr, dc), cp))
            return out

        def start_all(cps):
            for can_send, _, cp in cps:
                @pl.when(can_send)
                def _():
                    cp.start()

        def wait_recv_all(cps):
            for _, can_recv, cp in cps:
                @pl.when(can_recv)
                def _():
                    cp.wait_recv()

        def wait_send_all(cps):
            for can_send, _, cp in cps:
                @pl.when(can_send)
                def _():
                    cp.wait_send()

        def xcopies(t):
            return copies(sx.at[t], ecx.at[t], acx.at[t], xsend.at[t], xrecv.at[t])

        def hcopies(t):
            return copies(sh.at[t], ech.at[t], ach.at[t], hsend.at[t], hrecv.at[t])

        def shifted(v):
            n, channels = v.shape
            c_idx = lax.broadcasted_iota(jnp.int32, (1, W, channels), 1)
            left = jnp.where(c_idx == 0, 0.0, pltpu.roll(v, 1, 0).reshape(n // W, W, channels))
            right = jnp.where(c_idx == W - 1, 0.0, pltpu.roll(v, n - 1, 0).reshape(n // W, W, channels))
            return left.reshape(n, channels), right.reshape(n, channels)

        def put_rows(s_ref, v, first, lanes):
            left, right = shifted(v)
            for dx, form in enumerate((left, v, right)):
                s_ref[dx, pl.ds(first, v.shape[0]), lanes] = form.astype(jnp.bfloat16)

        def put_edges(ec_ref, j):
            for side in range(2):
                edge = hf[j, pl.ds(side * (W - 1), H * SEQ, stride=W), :]
                ec_ref[side, :, :, pl.ds(j * LANES, LANES)] = edge.astype(jnp.bfloat16).reshape(H, SEQ, LANES)

        def patch(s_ref, ac_ref, channels):
            i16 = lax.broadcasted_iota(jnp.int32, (16, channels), 0)
            for r in range(H):
                for side in range(2):
                    for s in range(SEQ):
                        pos = s * W if side == 0 else s * W + W - 1
                        base = PR * (r + 1) + pos // 16 * 16
                        dxi = 2 * side
                        old = s_ref[dxi, pl.ds(base, 16), :].astype(jnp.float32)
                        halo = ac_ref[side, r + 1, s:s + 1, :].astype(jnp.float32)
                        s_ref[dxi, pl.ds(base, 16), :] = jnp.where(i16 == pos % 16, halo, old).astype(jnp.bfloat16)
            pos_idx = lax.broadcasted_iota(jnp.int32, (PR, channels), 0)
            for r in (0, H + 1):
                v = s_ref[1, pl.ds(PR * r, PR), :].astype(jnp.float32)
                for side in range(2):
                    out = pltpu.roll(v, 1 if side == 0 else PR - 1, 0)
                    for s in range(SEQ):
                        halo = ac_ref[side, r, s:s + 1, :].astype(jnp.float32)
                        out = jnp.where(pos_idx == (s * W if side == 0 else s * W + W - 1), halo, out)
                    s_ref[2 * side, pl.ds(PR * r, PR), :] = out.astype(jnp.bfloat16)

        def gate_lanes(w_ref, rows, j):
            return jnp.concatenate([w_ref[rows, pl.ds(q * CH + j * LANES, LANES)] for q in range(4)], axis=1)

        def product(parts, j):
            lhs = [s_ref[k % 3, pl.ds(k // 3 * PR, M), :] for s_ref, _, _, taps in parts for k in taps]
            rhs = [gate_lanes(w_ref, pl.ds(k * n, n), j) for _, w_ref, n, taps in parts for k in taps]
            return jnp.dot(jnp.concatenate(lhs, axis=1), jnp.concatenate(rhs, axis=0), preferred_element_type=jnp.float32)

        def bias_block(j):
            return jnp.concatenate([bias[pl.ds(q * CH + j * LANES, LANES)].reshape(1, LANES) for q in range(4)], axis=1)

        ALL = tuple(range(9))
        CENTRE = (4,)
        OTHERS = (0, 1, 2, 3, 5, 6, 7, 8)

        def post(t, last):
            for j in range(NJ):
                lane = j * LANES
                gates = product([(sh.at[t], wh, CH, OTHERS)], j) + g[j]
                gi = sigmoid(gates[:, 0:LANES])
                gf = sigmoid(gates[:, LANES:2 * LANES])
                go = sigmoid(gates[:, 2 * LANES:3 * LANES])
                gg = jnp.tanh(gates[:, 3 * LANES:])
                c_old = cst[:, :, :, pl.ds(lane, LANES)].reshape(M, LANES)
                c_new = gf * c_old + gi * gg
                cst[:, :, :, pl.ds(lane, LANES)] = c_new.reshape(H, SEQ, W, LANES)
                h_new = go * jnp.tanh(c_new)
                h4 = h_new.reshape(H, SEQ, W, LANES)
                for s in range(SEQ):
                    ho[t, s, :, :, pl.ds(lane, LANES)] = h4[:, s].astype(jnp.bfloat16)
                if not last:
                    put_rows(sh.at[t + 1], h_new, PR, pl.ds(lane, LANES))
                    hf[j] = h_new
                    put_edges(ech.at[t + 1], j)

        def fill(raw, s_ref, ec_ref, channels):
            for r in range(H):
                v = raw[r].astype(jnp.float32).reshape(PR, channels)
                put_rows(s_ref, v, PR * (r + 1), slice(None))
                for k in range(channels // LANES):
                    hf[k, pl.ds(PR * r, PR), :] = v[:, k * LANES:(k + 1) * LANES]
            for k in range(channels // LANES):
                put_edges(ec_ref, k)

        for cp in xloads[0]:
            cp.wait()
        fill(rawx.at[0], sx.at[0], ecx.at[0], CX)
        n_near = sum(exists(dr, dc).astype(jnp.int32) for dr, dc in SLOTS)
        pl.semaphore_wait(barrier, n_near)
        start_all(xcopies(0))
        for cp in hloads:
            cp.wait()
        fill(rawh, sh.at[0], ech.at[0], CH)
        start_all(hcopies(0))
        for cp in (bload, wxloads[0], whloads[0]):
            cp.wait()
        for j in range(NJ):
            g[j] = product([(sx.at[0], wx, CX, CENTRE), (sh.at[0], wh, CH, CENTRE)], j) + bias_block(j)
        for t in range(1, T):
            for cp in xloads[t]:
                cp.wait()

        @pl.loop(1, T)
        def _(t):
            fill(rawx.at[t], sx.at[t], ecx.at[t], CX)
            start_all(xcopies(t))

        for cp in (*cloads, *wxloads[1:]):
            cp.wait()
        wait_recv_all(xcopies(0))
        wait_send_all(xcopies(0))
        patch(sx.at[0], acx.at[0], CX)
        for j in range(NJ):
            g[j] += product([(sx.at[0], wx, CX, OTHERS)], j)
        for cp in whloads[1:]:
            cp.wait()

        @pl.loop(0, T - 1)
        def _(t):
            wait_recv_all(hcopies(t))
            wait_send_all(hcopies(t))
            wait_recv_all(xcopies(t + 1))
            wait_send_all(xcopies(t + 1))
            patch(sh.at[t], ach.at[t], CH)
            post(t, False)
            patch(sx.at[t + 1], acx.at[t + 1], CX)
            start_all(hcopies(t + 1))
            for j in range(NJ):
                g[j] = product([(sx.at[t + 1], wx, CX, ALL), (sh.at[t + 1], wh, CH, CENTRE)], j) + bias_block(j)

        wait_recv_all(hcopies(T - 1))
        wait_send_all(hcopies(T - 1))
        patch(sh.at[T - 1], ach.at[T - 1], CH)
        post(T - 1, True)

    return kernel


def solution(mesh):
    row_count = mesh.shape["rows"]
    col_count = mesh.shape["cols"]
    frame_spec = P(None, "batch", "rows", "cols", None)
    state_spec = P("batch", "rows", "cols", None)

    def local_run(frames, w_x, w_h, gate_bias, h_init, c_init):
        T, SEQ, H, W, CX = frames.shape
        CH = h_init.shape[-1]
        NG = 4 * CH
        PR = SEQ * W
        M = H * PR
        bf, f32 = jnp.bfloat16, jnp.float32
        hbm = pl.BlockSpec(memory_space=pl.ANY)
        vmem = pl.BlockSpec(memory_space=pltpu.VMEM)
        kernel = make_kernel((T, SEQ, H, W, CX, CH), row_count, col_count)
        h_vmem, c_vmem = pl.pallas_call(
            kernel,
            out_shape=(pltpu.VMEM((T, SEQ, H, W, CH), bf), pltpu.VMEM((H, SEQ, W, CH), f32)),
            in_specs=[hbm] * 6,
            out_specs=(vmem, vmem),
            scratch_shapes=[
                pltpu.VMEM((9 * CX, NG), bf), pltpu.VMEM((9 * CH, NG), bf), pltpu.VMEM((NG,), f32),
                pltpu.VMEM((T, H, SEQ, W, CX), bf), pltpu.VMEM((H, SEQ, W, CH), bf),
                pltpu.VMEM((T, 3, M + 2 * PR, CX), bf), pltpu.VMEM((T, 3, M + 2 * PR, CH), bf),
                pltpu.VMEM((CH // LANES, M, 4 * LANES), f32), pltpu.VMEM((max(CH, CX) // LANES, M, LANES), f32),
                pltpu.VMEM((T, 2, H, SEQ, CX), bf), pltpu.VMEM((T, 2, H, SEQ, CH), bf),
                pltpu.VMEM((T, 2, H + 2, SEQ, CX), bf), pltpu.VMEM((T, 2, H + 2, SEQ, CH), bf),
                pltpu.SemaphoreType.DMA((7,)), pltpu.SemaphoreType.DMA((T + 2, SEQ)),
                pltpu.SemaphoreType.DMA((T, 8)), pltpu.SemaphoreType.DMA((T, 8)),
                pltpu.SemaphoreType.DMA((T, 8)), pltpu.SemaphoreType.DMA((T, 8)),
            ],
            compiler_params=pltpu.CompilerParams(
                collective_id=0, has_side_effects=True, vmem_limit_bytes=56 * 1024 * 1024),
        )(frames, w_x.reshape(9 * CX, NG), w_h.reshape(9 * CH, NG), gate_bias, h_init, c_init)

        def write_out(h_ref, c_ref, h_out, c_out, sem):
            cps = [pltpu.make_async_copy(h_ref, h_out, sem.at[SEQ])]
            cps += [pltpu.make_async_copy(c_ref.at[:, s], c_out.at[s], sem.at[s]) for s in range(SEQ)]
            for cp in cps:
                cp.start()
            for cp in cps:
                cp.wait()

        return pl.pallas_call(
            write_out,
            out_shape=(jax.ShapeDtypeStruct((T, SEQ, H, W, CH), bf), jax.ShapeDtypeStruct((SEQ, H, W, CH), f32)),
            in_specs=[vmem] * 2,
            out_specs=(hbm, hbm),
            scratch_shapes=[pltpu.SemaphoreType.DMA((SEQ + 1,))],
            compiler_params=pltpu.CompilerParams(vmem_limit_bytes=1024 * 1024),
        )(h_vmem, c_vmem)

    return jax.shard_map(local_run, mesh=mesh,
                         in_specs=(frame_spec, P(), P(), P(), state_spec, state_spec),
                         out_specs=(frame_spec, state_spec), check_vma=False)
```

```python
import jax
import jax.numpy as jnp
from jax import lax
from jax.experimental import pallas as pl
from jax.experimental.pallas import tpu as pltpu
from jax.sharding import PartitionSpec as P

MESH = pl.DeviceIdType.MESH
LANES = 128
SLOTS = ((-1, 0), (1, 0), (0, -1), (0, 1), (-1, -1), (-1, 1), (1, -1), (1, 1))


def sigmoid(x):
    return 0.5 * jnp.tanh(0.5 * x) + 0.5


def make_kernel(dims, row_count, col_count):
    T, SEQ, H, W, CX, CH = dims
    PR = SEQ * W
    M = H * PR
    NJ = CH // LANES

    def kernel(frames, wx_hbm, wh_hbm, bias_hbm, h_init, c_init, ho, cst,
               wx, wh, bias, rawx, rawh, sx, sh, g, hf, ecx, ech, acx, ach,
               wsem, rsem, send, recv):
        b = lax.axis_index("batch")
        row = lax.axis_index("rows")
        col = lax.axis_index("cols")

        def exists(dr, dc):
            r, c = row + dr, col + dc
            return (r >= 0) & (r < row_count) & (c >= 0) & (c < col_count)

        barrier = pltpu.get_barrier_semaphore()
        for dr, dc in SLOTS:
            @pl.when(exists(dr, dc))
            def _():
                pl.semaphore_signal(barrier, inc=1, device_id=(b, col + dc, row + dr), device_id_type=MESH)

        xloads = [[pltpu.make_async_copy(frames.at[t, s], rawx.at[t, :, s], rsem.at[t, s]) for s in range(SEQ)]
                  for t in range(T)]
        hloads = [pltpu.make_async_copy(h_init.at[s], rawh.at[:, s], rsem.at[T, s]) for s in range(SEQ)]
        cloads = [pltpu.make_async_copy(c_init.at[s], cst.at[:, s], rsem.at[T + 1, s]) for s in range(SEQ)]
        bload = pltpu.make_async_copy(bias_hbm, bias, wsem.at[0])

        def wloads(w_hbm, w_vmem, channels, first_sem):
            parts = (pl.ds(4 * channels, channels), pl.ds(0, 4 * channels), pl.ds(5 * channels, 4 * channels))
            return [pltpu.make_async_copy(w_hbm.at[p], w_vmem.at[p], wsem.at[first_sem + i]) for i, p in enumerate(parts)]
        wxloads = wloads(wx_hbm, wx, CX, 1)
        whloads = wloads(wh_hbm, wh, CH, 4)
        later = [cp for t in range(1, T) for cp in xloads[t]]
        for cp in [*xloads[0], *hloads, bload, wxloads[0], whloads[0], *later, *wxloads[1:], *cloads, *whloads[1:]]:
            cp.start()

        def zero(cond, refs):
            @pl.when(cond)
            def _():
                for ref in refs:
                    ref[...] = jnp.zeros(ref.shape, ref.dtype)
        zero(row == 0, [sx.at[:, 1, 0:PR], sh.at[:, 1, 0:PR], acx.at[:, :, 0], ach.at[:, :, 0]])
        zero(row == row_count - 1, [sx.at[:, 1, M + PR:M + 2 * PR], sh.at[:, 1, M + PR:M + 2 * PR],
                                    acx.at[:, :, H + 1], ach.at[:, :, H + 1]])
        zero(col == 0, [acx.at[:, 0], ach.at[:, 0]])
        zero(col == col_count - 1, [acx.at[:, 1], ach.at[:, 1]])

        def copies(lead, s_all, ec_all, ac_all, sem_set):
            parts = ((s_all.at[lead, 1, pl.ds(M, PR)], s_all.at[lead, 1, pl.ds(0, PR)]),
                     (s_all.at[lead, 1, pl.ds(PR, PR)], s_all.at[lead, 1, pl.ds(M + PR, PR)]),
                     (ec_all.at[lead, 1], ac_all.at[lead, 0, pl.ds(1, H)]),
                     (ec_all.at[lead, 0], ac_all.at[lead, 1, pl.ds(1, H)]),
                     (ec_all.at[lead, 1, H - 1], ac_all.at[lead, 0, 0]),
                     (ec_all.at[lead, 0, H - 1], ac_all.at[lead, 1, 0]),
                     (ec_all.at[lead, 1, 0], ac_all.at[lead, 0, H + 1]),
                     (ec_all.at[lead, 0, 0], ac_all.at[lead, 1, H + 1]))
            out = []
            for i, (dr, dc) in enumerate(SLOTS):
                cp = pltpu.make_async_remote_copy(
                    src_ref=parts[i][0], dst_ref=parts[i][1],
                    send_sem=send.at[sem_set, i], recv_sem=recv.at[sem_set, i],
                    device_id=(b, col - dc, row - dr), device_id_type=MESH)
                out.append((exists(-dr, -dc), exists(dr, dc), cp))
            return out

        def start_all(cps):
            for can_send, _, cp in cps:
                @pl.when(can_send)
                def _():
                    cp.start()

        def wait_recv_all(cps):
            for _, can_recv, cp in cps:
                @pl.when(can_recv)
                def _():
                    cp.wait_recv()

        def wait_send_all(cps):
            for can_send, _, cp in cps:
                @pl.when(can_send)
                def _():
                    cp.wait_send()

        def x_first():
            return copies(0, sx, ecx, acx, 2)

        def x_rest():
            return copies(pl.ds(1, T - 1), sx, ecx, acx, 3)

        def hcopies(t):
            return copies(t, sh, ech, ach, lax.rem(t, 3))

        def shifted(v):
            n, channels = v.shape
            c_idx = lax.broadcasted_iota(jnp.int32, (1, W, channels), 1)
            left = jnp.where(c_idx == 0, 0.0, pltpu.roll(v, 1, 0).reshape(n // W, W, channels))
            right = jnp.where(c_idx == W - 1, 0.0, pltpu.roll(v, n - 1, 0).reshape(n // W, W, channels))
            return left.reshape(n, channels), right.reshape(n, channels)

        def put_rows(s_ref, v, first, lanes):
            left, right = shifted(v)
            for dx, form in enumerate((left, v, right)):
                s_ref[dx, pl.ds(first, v.shape[0]), lanes] = form.astype(jnp.bfloat16)

        def put_edges(ec_ref, j):
            for side in range(2):
                edge = hf[j, pl.ds(side * (W - 1), H * SEQ, stride=W), :]
                ec_ref[side, :, :, pl.ds(j * LANES, LANES)] = edge.astype(jnp.bfloat16).reshape(H, SEQ, LANES)

        def patch(s_ref, ac_ref, channels):
            i16 = lax.broadcasted_iota(jnp.int32, (16, channels), 0)
            for r in range(H):
                for side in range(2):
                    for s in range(SEQ):
                        pos = s * W if side == 0 else s * W + W - 1
                        base = PR * (r + 1) + pos // 16 * 16
                        dxi = 2 * side
                        old = s_ref[dxi, pl.ds(base, 16), :].astype(jnp.float32)
                        halo = ac_ref[side, r + 1, s:s + 1, :].astype(jnp.float32)
                        s_ref[dxi, pl.ds(base, 16), :] = jnp.where(i16 == pos % 16, halo, old).astype(jnp.bfloat16)
            pos_idx = lax.broadcasted_iota(jnp.int32, (PR, channels), 0)
            for r in (0, H + 1):
                v = s_ref[1, pl.ds(PR * r, PR), :].astype(jnp.float32)
                for side in range(2):
                    out = pltpu.roll(v, 1 if side == 0 else PR - 1, 0)
                    for s in range(SEQ):
                        halo = ac_ref[side, r, s:s + 1, :].astype(jnp.float32)
                        out = jnp.where(pos_idx == (s * W if side == 0 else s * W + W - 1), halo, out)
                    s_ref[2 * side, pl.ds(PR * r, PR), :] = out.astype(jnp.bfloat16)

        def gate_lanes(w_ref, rows, j):
            return jnp.concatenate([w_ref[rows, pl.ds(q * CH + j * LANES, LANES)] for q in range(4)], axis=1)

        def product(parts, j, first_row=0, rows=H):
            lhs = [s_ref[k % 3, pl.ds((k // 3 + first_row) * PR, rows * PR), :] for s_ref, _, _, taps in parts for k in taps]
            rhs = [gate_lanes(w_ref, pl.ds(k * n, n), j) for _, w_ref, n, taps in parts for k in taps]
            return jnp.dot(jnp.concatenate(lhs, axis=1), jnp.concatenate(rhs, axis=0), preferred_element_type=jnp.float32)

        def bias_block(j):
            return jnp.concatenate([bias[pl.ds(q * CH + j * LANES, LANES)].reshape(1, LANES) for q in range(4)], axis=1)

        CENTRE = (4,)
        EARLY = (1, 7, 0)
        LATE = (3, 6, 2, 5, 8)

        def cell(t, j, gates, first_row, rows, last):
            lanes = pl.ds(j * LANES, LANES)
            grid_rows = pl.ds(first_row, rows)
            gi = sigmoid(gates[:, 0:LANES])
            gf = sigmoid(gates[:, LANES:2 * LANES])
            go = sigmoid(gates[:, 2 * LANES:3 * LANES])
            gg = jnp.tanh(gates[:, 3 * LANES:])
            c_old = cst[grid_rows, :, :, lanes].reshape(rows * PR, LANES)
            c_new = gf * c_old + gi * gg
            cst[grid_rows, :, :, lanes] = c_new.reshape(rows, SEQ, W, LANES)
            h_new = go * jnp.tanh(c_new)
            h4 = h_new.reshape(rows, SEQ, W, LANES)
            for s in range(SEQ):
                ho[t, s, grid_rows, :, lanes] = h4[:, s].astype(jnp.bfloat16)
            if not last:
                put_rows(sh.at[t + 1], h_new, PR, lanes)
                hf[j] = h_new
                put_edges(ech.at[t + 1], j)

        def post(t, last):
            for j in range(NJ):
                halves = 2 if last and j == NJ - 1 else 1
                rows = H // halves
                for half in range(halves):
                    first = half * rows
                    gates = product([(sh.at[t], wh, CH, EARLY + LATE)], j, first, rows) + g[t, j, pl.ds(first * PR, rows * PR), :]
                    if not last and j == NJ - 1:
                        g[t + 1, 0] += product([(sx.at[t + 1], wx, CX, EARLY)], 0)
                    cell(t, j, gates, first, rows, last)

        def fill(raw, s_ref, ec_ref, channels):
            for r in range(H):
                v = raw[r].astype(jnp.float32).reshape(PR, channels)
                put_rows(s_ref, v, PR * (r + 1), slice(None))
                for k in range(channels // LANES):
                    hf[k, pl.ds(PR * r, PR), :] = v[:, k * LANES:(k + 1) * LANES]
            for k in range(channels // LANES):
                put_edges(ec_ref, k)

        for cp in xloads[0]:
            cp.wait()
        fill(rawx.at[0], sx.at[0], ecx.at[0], CX)
        n_near = sum(exists(dr, dc).astype(jnp.int32) for dr, dc in SLOTS)
        pl.semaphore_wait(barrier, n_near)
        start_all(x_first())
        for cp in hloads:
            cp.wait()
        fill(rawh, sh.at[0], ech.at[0], CH)
        start_all(hcopies(0))
        for cp in (bload, wxloads[0], whloads[0], *later):
            cp.wait()
        for j in range(NJ):
            g[0, j] = product([(sx.at[0], wx, CX, CENTRE), (sh.at[0], wh, CH, CENTRE)], j) + bias_block(j)
        for t in range(1, T):
            fill(rawx.at[t], sx.at[t], ecx.at[t], CX)
        start_all(x_rest())
        for t in range(1, T):
            for j in range(NJ):
                g[t, j] = product([(sx.at[t], wx, CX, CENTRE)], j) + bias_block(j)

        for cp in (*cloads, *wxloads[1:]):
            cp.wait()
        wait_recv_all(x_first())
        wait_send_all(x_first())
        patch(sx.at[0], acx.at[0], CX)
        for j in range(NJ):
            g[0, j] += product([(sx.at[0], wx, CX, EARLY + LATE)], j)
        for cp in whloads[1:]:
            cp.wait()
        wait_recv_all(x_rest())
        wait_send_all(x_rest())

        @pl.loop(0, T - 1)
        def _(t):
            wait_recv_all(hcopies(t))
            wait_send_all(hcopies(t))
            patch(sh.at[t], ach.at[t], CH)
            patch(sx.at[t + 1], acx.at[t + 1], CX)
            post(t, False)
            start_all(hcopies(t + 1))
            for j in range(NJ):
                x_taps = LATE if j == 0 else EARLY + LATE
                g[t + 1, j] += product([(sx.at[t + 1], wx, CX, x_taps), (sh.at[t + 1], wh, CH, CENTRE)], j)

        wait_recv_all(hcopies(T - 1))
        wait_send_all(hcopies(T - 1))
        patch(sh.at[T - 1], ach.at[T - 1], CH)
        post(T - 1, True)

    return kernel


def solution(mesh):
    row_count = mesh.shape["rows"]
    col_count = mesh.shape["cols"]
    frame_spec = P(None, "batch", "rows", "cols", None)
    state_spec = P("batch", "rows", "cols", None)

    def local_run(frames, w_x, w_h, gate_bias, h_init, c_init):
        T, SEQ, H, W, CX = frames.shape
        CH = h_init.shape[-1]
        NG = 4 * CH
        PR = SEQ * W
        M = H * PR
        bf, f32 = jnp.bfloat16, jnp.float32
        hbm = pl.BlockSpec(memory_space=pl.ANY)
        vmem = pl.BlockSpec(memory_space=pltpu.VMEM)
        kernel = make_kernel((T, SEQ, H, W, CX, CH), row_count, col_count)
        h_vmem, c_vmem = pl.pallas_call(
            kernel,
            out_shape=(pltpu.VMEM((T, SEQ, H, W, CH), bf), pltpu.VMEM((H, SEQ, W, CH), f32)),
            in_specs=[hbm] * 6,
            out_specs=(vmem, vmem),
            scratch_shapes=[
                pltpu.VMEM((9 * CX, NG), bf), pltpu.VMEM((9 * CH, NG), bf), pltpu.VMEM((NG,), f32),
                pltpu.VMEM((T, H, SEQ, W, CX), bf), pltpu.VMEM((H, SEQ, W, CH), bf),
                pltpu.VMEM((T, 3, M + 2 * PR, CX), bf), pltpu.VMEM((T, 3, M + 2 * PR, CH), bf),
                pltpu.VMEM((T, CH // LANES, M, 4 * LANES), f32), pltpu.VMEM((max(CH, CX) // LANES, M, LANES), f32),
                pltpu.VMEM((T, 2, H, SEQ, CX), bf), pltpu.VMEM((T, 2, H, SEQ, CH), bf),
                pltpu.VMEM((T, 2, H + 2, SEQ, CX), bf), pltpu.VMEM((T, 2, H + 2, SEQ, CH), bf),
                pltpu.SemaphoreType.DMA((7,)), pltpu.SemaphoreType.DMA((T + 2, SEQ)),
                pltpu.SemaphoreType.DMA((4, 8)), pltpu.SemaphoreType.DMA((4, 8)),
            ],
            compiler_params=pltpu.CompilerParams(
                collective_id=0, has_side_effects=True, vmem_limit_bytes=56 * 1024 * 1024),
        )(frames, w_x.reshape(9 * CX, NG), w_h.reshape(9 * CH, NG), gate_bias, h_init, c_init)

        def write_out(h_ref, c_ref, h_out, c_out, sem):
            cps = [pltpu.make_async_copy(h_ref, h_out, sem.at[SEQ])]
            cps += [pltpu.make_async_copy(c_ref.at[:, s], c_out.at[s], sem.at[s]) for s in range(SEQ)]
            for cp in cps:
                cp.start()
            for cp in cps:
                cp.wait()

        return pl.pallas_call(
            write_out,
            out_shape=(jax.ShapeDtypeStruct((T, SEQ, H, W, CH), bf), jax.ShapeDtypeStruct((SEQ, H, W, CH), f32)),
            in_specs=[vmem] * 2,
            out_specs=(hbm, hbm),
            scratch_shapes=[pltpu.SemaphoreType.DMA((SEQ + 1,))],
            compiler_params=pltpu.CompilerParams(vmem_limit_bytes=1024 * 1024),
        )(h_vmem, c_vmem)

    return jax.shard_map(local_run, mesh=mesh,
                         in_specs=(frame_spec, P(), P(), P(), state_spec, state_spec),
                         out_specs=(frame_spec, state_spec), check_vma=False)
```
